32 devices in a mesh: expert: 4 (over y, x), ffn: 8 (over z, core).
Axes of the slice: x: 2, y: 2, z: 4, core: 2. Of those that a mesh axis runs over, the one named last changes fastest.
Arguments:
- tokens: bfloat16 [1024, 4096], P('expert'), may hold values from -6 to 6
- router_gates: float32 [1024, 2], P('expert'), may hold values from 0.1 to 1
- routes: int32 [1024, 2], P('expert'), may hold values from 0 to 3, all different within a row; in each aligned block of 256 rows (0 to 255, 256 to 511, ...) at most 256 rows name the same one
- gate_proj: bfloat16 [4, 4096, 14336], P('expert', None, 'ffn'), may hold values from -0.09375 to 0.09375
- up_proj: bfloat16 [4, 4096, 14336], P('expert', None, 'ffn'), may hold values from -0.09375 to 0.09375
- down_proj: bfloat16 [4, 14336, 4096], P('expert', 'ffn'), may hold values from -0.0625 to 0.0625
Outputs:
- mixed: bfloat16 [1024, 4096], P('expert', 'ffn')
The draws below stay inside these ranges and needn't reach their ends.
Inputs may be any that keep to these rules, and one draw needn't show every extreme that they name: `routes`: the 2 experts of a token differ. Among the tokens of one index of the expert axis (aligned blocks of 256 tokens) no expert is chosen by more than 256 tokens, and in some blocks one expert is chosen by exactly 256.
All inputs are finite; a program needn't handle non-finite values.
Results may differ from the reference program's by a relative error of at most 0.017.
Values may be sent and summed in bfloat16 or wider, within the bound.
A program may use at most 128 MiB of HBM per device.

```python
import math
import jax
import jax.numpy as jnp
import numpy as np
from jax import lax

D = 4096
FF = 14336
TOP = 2
TOK_DEV = 256
EXPERTS = 4
CAP = 256
TOKENS = 1024
N_FFN = 8


def strengthened(values, rng, source, target, parts, factor):
    def block_of(dim):
        return (jnp.arange(values.shape[dim]) // (values.shape[dim] // parts)).reshape((-1,) + (1,) * (values.ndim - 1 - dim))

    one_side = jax.random.permutation(rng, parts)[block_of(target)]
    other_side = (block_of(target) + parts // 2) % parts
    return jnp.where((block_of(source) == one_side) | (block_of(source) == other_side), factor * values, values)


def steps_of(key, dims, pieces, low, high):
    loudness = 1.0
    for axis_at, shards_of in pieces:
        steps = jax.random.uniform(jax.random.fold_in(jax.random.fold_in(key, 6), axis_at), (shards_of,), jnp.float32, low / len(pieces), high / len(pieces))
        loudness = loudness * jnp.repeat(jnp.exp(steps), dims[axis_at] // shards_of).reshape((-1,) + (1,) * (len(dims) - 1 - axis_at))
    return loudness


def shared_out(key, own, number, rows, count, top, limit, lean):
    sequence = jax.random.permutation(key, count)
    crowded, ordinary = load_shares(count, rows * top, limit, lean, True), load_shares(count, rows * top, limit, lean, False)
    places = jnp.arange(count)

    def named(lengths, offset_by):
        used = int((lengths > 0).sum())
        fixed = max(1, used // 4)
        passed = fixed + (places - fixed + offset_by * (used - fixed)) % max(1, count - fixed)
        return jnp.zeros((count,), jnp.int32).at[sequence[jnp.where(places < fixed, places, passed)]].set(jnp.asarray(lengths, jnp.int32))

    lengths = jnp.where(number % 4 == 0, named(crowded, number // 4), named(ordinary, number - number // 4 - 1))
    mixed = jax.random.permutation(jax.random.fold_in(own, 3), count)
    source_of, taker = mixed[0:count // 2 * 2:2], mixed[1:count // 2 * 2:2]
    slack = jnp.minimum(lengths[source_of] - 1, limit - lengths[taker]) // 2
    slack = jnp.where((source_of == sequence[0]) | (taker == sequence[0]) | (lengths[taker] == 0), 0, jnp.maximum(slack, 0))
    passed = jax.random.randint(jax.random.fold_in(own, 4), (count // 2,), 0, 1 << 20) % (slack + 1)
    lengths = lengths.at[source_of].add(-passed).at[taker].add(passed)
    labels = jnp.searchsorted(jnp.cumsum(lengths), jnp.arange(rows * top), side="right").astype(jnp.int32)
    grid = labels.reshape(top, rows).T
    grid = grid[jax.random.permutation(jax.random.fold_in(own, 1), rows)]
    offset_by = jax.random.randint(jax.random.fold_in(own, 2), (rows, 1), 0, top)
    return jnp.take_along_axis(grid, (jnp.arange(top)[None, :] + offset_by) % top, axis=1)


def load_shares(number_of, total, reach, lean, full):
    weights = [(1 << 20) // math.isqrt(standing ** lean) + 1 for standing in range(1, number_of + 1)]
    largest = reach if full else min(reach, max(-(-total // number_of), total * weights[0] // sum(weights)))
    least = 1 if total - largest >= number_of - 1 else 0
    holding, surplus = [largest] + [least] * (number_of - 1), total - largest - least * (number_of - 1)
    while surplus > 0:
        free = [i for i in range(1, number_of) if holding[i] < largest] or [i for i in range(1, number_of) if holding[i] < reach]
        pool, budget = sum([weights[i] for i in free]), surplus
        for i in free:
            extra = min(reach - holding[i], max(1, budget * weights[i] // pool), surplus)
            holding[i] = holding[i] + extra
            surplus = surplus - extra
    return np.array(holding)


def centred(own_key, shape, deviation, most, shards=(), kind=jnp.bfloat16):
    entries = deviation * jax.random.normal(own_key, shape, jnp.float32)
    if shards:
        entries = entries * steps_of(own_key, shape, shards, -0.22, 0.18)
    return jnp.clip(entries, -most, most).astype(kind)


def gaussian_with(own_key, extent, spread, bound, cuts, heavy, kind=jnp.bfloat16):
    drawn = spread * jax.random.normal(own_key, extent, jnp.float32)
    if cuts:
        drawn = drawn * steps_of(own_key, extent, cuts, -0.22, 0.18)
    return jnp.clip(strengthened(drawn, jax.random.fold_in(own_key, 3), *heavy), -bound, bound).astype(kind)


def setup_inputs(seed: int = 0) -> dict:
    streams_of = jax.random.split(jax.random.key(seed), 7)
    tokens = centred(streams_of[0], (TOKENS, D), 1.0, 6.0, ((0, 4),))
    router_gates = jnp.clip(jnp.exp(math.log(1.0) - 2.3025851 * jax.random.uniform(streams_of[1], (TOKENS, TOP), jnp.float32) ** steps_of(streams_of[1], (TOKENS, TOP), ((0, 4),), -0.2, 0.2)), 0.1, 1.0)
    routes_keys = jax.random.split(jax.random.fold_in(streams_of[2], 1), TOKENS // TOK_DEV)
    routes_turns = jax.random.permutation(jax.random.fold_in(streams_of[2], 3), TOKENS // TOK_DEV)
    routes = jax.vmap(lambda own, number: shared_out(jax.random.fold_in(streams_of[2], 2), own, number, TOK_DEV, EXPERTS, TOP, CAP, 2))(routes_keys, routes_turns).reshape((TOKENS, TOP))
    gate_proj = centred(streams_of[3], (EXPERTS, D, FF), D ** -0.5, 0.09375, ((0, 4), (2, 8)))
    up_proj = centred(streams_of[4], (EXPERTS, D, FF), D ** -0.5, 0.09375, ((0, 4), (2, 8)))
    down_proj = gaussian_with(streams_of[5], (EXPERTS, FF, D), FF ** -0.5, 0.0625, ((0, 4), (1, 8)), (1, 2, 8, 2.0))
    return {"tokens": tokens, "router_gates": router_gates, "routes": routes, "gate_proj": gate_proj, "up_proj": up_proj, "down_proj": down_proj}


def slot_numbers(routes):
    grouped = routes.reshape(-1, TOK_DEV * TOP)
    chosen = (grouped[:, :, None] == jnp.arange(EXPERTS, dtype=jnp.int32)[None, None, :]).astype(jnp.int32)
    ranking = jnp.cumsum(chosen, axis=1) - chosen
    return jnp.sum(ranking * chosen, axis=2).reshape(-1, TOP).astype(jnp.int32)


def run_expert(operands):
    buffer_rows, gate_matrix, up_matrix, down_matrix = operands
    gate_act = jnp.dot(buffer_rows, gate_matrix, preferred_element_type=jnp.float32)
    up_act = jnp.dot(buffer_rows, up_matrix, preferred_element_type=jnp.float32)
    hidden = (jax.nn.silu(gate_act) * up_act).astype(jnp.bfloat16)
    shard_width = FF // N_FFN

    def add_shard(running, shard_index):
        hidden_part = lax.dynamic_slice_in_dim(hidden, shard_index * shard_width, shard_width, 1)
        down_part = lax.dynamic_slice_in_dim(down_matrix, shard_index * shard_width, shard_width, 0)
        rounded = jnp.dot(hidden_part, down_part, preferred_element_type=jnp.float32).astype(jnp.bfloat16)
        rounded = lax.optimization_barrier(rounded)
        return running + rounded.astype(jnp.float32), None

    start_sum = jnp.zeros((buffer_rows.shape[0], D), jnp.float32)
    result, unused = lax.scan(add_shard, start_sum, jnp.arange(N_FFN, dtype=jnp.int32))
    return result


def reference(tokens, router_gates, routes, gate_proj, up_proj, down_proj):
    sources = TOKENS // TOK_DEV
    slot = slot_numbers(routes)
    owner = (jnp.arange(TOKENS, dtype=jnp.int32) // TOK_DEV)[:, None]
    position = (owner * CAP + slot).astype(jnp.int32)
    buffers = jnp.zeros((EXPERTS, sources * CAP, D), jnp.bfloat16)
    buffers = buffers.at[routes, position].set(jnp.broadcast_to(tokens[:, None, :], (TOKENS, TOP, D)))
    outputs = lax.map(run_expert, (buffers, gate_proj, up_proj, down_proj))
    picked = outputs[routes, position]
    mixed = jnp.sum(router_gates[:, :, None] * picked, axis=1)
    return mixed.astype(jnp.bfloat16)
```

```python
import functools

import jax
import jax.numpy as jnp
from jax import lax
from jax.experimental import pallas as pl
from jax.experimental.pallas import tpu as pltpu
from jax.sharding import PartitionSpec as P


def swap(value, axis, bit):
    size = lax.axis_size(axis)
    return lax.ppermute(value, axis, [(i, i ^ bit) for i in range(size)])


def after(value, *others):
    return lax.optimization_barrier((value,) + others)[0]


def expert_kernel(blocks, core_ref, x_ref, w_ref, gate_ref, up_ref, down_ref, keep_ref, give_ref, acc):
    step = pl.program_id(0)

    @pl.when(step == 0)
    def clear():
        acc[...] = jnp.zeros_like(acc)

    gate_act = jnp.dot(x_ref[...], gate_ref[...], preferred_element_type=jnp.float32)
    up_act = jnp.dot(x_ref[...], up_ref[...], preferred_element_type=jnp.float32)
    hidden = gate_act / (1.0 + jnp.exp(-gate_act)) * up_act * w_ref[...]
    acc[...] += jnp.dot(
        hidden.astype(jnp.bfloat16), down_ref[...], preferred_element_type=jnp.float32
    )

    @pl.when(step == pl.num_programs(0) - 1)
    def write():
        core = core_ref[0]
        size = acc.shape[1] // (2 * blocks)
        for b in range(blocks):
            here = pl.ds(b * size, size)
            own = pl.ds(pl.multiple_of((2 * b + core) * size, size), size)
            far = pl.ds(pl.multiple_of((2 * b + 1 - core) * size, size), size)
            keep_ref[:, here] = acc[:, own].astype(keep_ref.dtype)
            give_ref[:, here] = acc[:, far].astype(give_ref.dtype)


def run_expert(core, x, weight, gate_matrix, up_matrix, down_matrix, blocks):
    rows, width = x.shape
    hidden = gate_matrix.shape[1]
    tile = 256 if hidden % 256 == 0 else 128
    half = jax.ShapeDtypeStruct((rows, width // 2), jnp.bfloat16)
    return pl.pallas_call(
        functools.partial(expert_kernel, blocks),
        out_shape=(half, half),
        grid_spec=pltpu.PrefetchScalarGridSpec(
            num_scalar_prefetch=1,
            grid=(hidden // tile,),
            in_specs=[
                pl.BlockSpec((rows, width), lambda i, c: (0, 0)),
                pl.BlockSpec((rows, 1), lambda i, c: (0, 0)),
                pl.BlockSpec((width, tile), lambda i, c: (0, i)),
                pl.BlockSpec((width, tile), lambda i, c: (0, i)),
                pl.BlockSpec((tile, width), lambda i, c: (i, 0)),
            ],
            out_specs=[pl.BlockSpec((rows, width // 2), lambda i, c: (0, 0))] * 2,
            scratch_shapes=[pltpu.VMEM((rows, width), jnp.float32)],
        ),
        compiler_params=pltpu.CompilerParams(
            dimension_semantics=("arbitrary",), vmem_limit_bytes=48 * 1024 * 1024
        ),
        cost_estimate=pl.CostEstimate(
            flops=6 * rows * width * hidden,
            bytes_accessed=6 * width * hidden,
            transcendentals=rows * hidden,
        ),
    )(core, x, weight, gate_matrix, up_matrix, down_matrix)


def groups_of(experts):
    steps = list(range(experts))
    return [steps[:1]] + [steps[i : i + 2] for i in range(1, experts - 1, 2)] + [steps[-1:]]


def per_device(tokens, router_gates, routes, gate_proj, up_proj, down_proj):
    experts = lax.axis_size("expert")
    groups = lax.axis_size("ffn")
    rows, width = tokens.shape
    col_width = width // groups
    blocks = groups // 2
    half_rows = rows // 2
    me = lax.axis_index("expert")
    group = lax.axis_index("ffn")
    core = group % 2
    block = group // 2
    core_word = jnp.full((1,), core, jnp.int32)
    gate_matrix, up_matrix, down_matrix = gate_proj[0], up_proj[0], down_proj[0]

    routes_t, gates_t = routes.T, router_gates.T
    names = jnp.arange(experts, dtype=jnp.int32)[:, None]
    dense = sum(
        jnp.where(routes_t[k][None, :] == names, gates_t[k][None, :], 0.0)
        for k in range(routes.shape[1])
    )

    half = lax.dynamic_slice_in_dim(tokens, core * half_rows, half_rows, 0)
    first_steps = list(range(1, experts))[:2]
    fetched, paired = {}, {}
    for step in first_steps:
        fetched[step] = swap(half, "expert", step)
    for step in first_steps:
        paired[step] = swap(fetched[step], "ffn", 1)
    for step in range(3, experts):
        source = after(half, *[paired[s] for s in first_steps])
        fetched[step] = swap(source, "expert", step)
    weights = {0: lax.dynamic_index_in_dim(dense, me, 0, keepdims=False)}
    for step in range(1, experts):
        column = lax.dynamic_index_in_dim(dense, me ^ step, 0, keepdims=False)
        weights[step] = swap(column, "expert", step)

    def chunk_of(steps):
        if steps == [0]:
            return tokens
        parts = []
        for step in steps:
            mine = fetched[step]
            other = paired[step] if step in paired else swap(mine, "ffn", 1)
            parts += [jnp.where(core == 0, mine, other), jnp.where(core == 0, other, mine)]
        return jnp.concatenate(parts, axis=0)

    parts = 2
    size = rows // parts
    returned, previous = [], None
    every = groups_of(experts)
    for number, steps in enumerate(every):
        chunk = chunk_of(steps)
        if number > 1:
            chunk = after(chunk, previous)
        weight = jnp.concatenate([weights[s] for s in steps])[:, None]
        keep, give = run_expert(
            core_word, chunk, weight, gate_matrix, up_matrix, down_matrix, blocks
        )
        got = swap(give, "ffn", 1)
        total = (keep.astype(jnp.float32) + got.astype(jnp.float32)).astype(jnp.bfloat16)
        previous = total
        for at, step in enumerate(steps):
            mine = total[at * rows : (at + 1) * rows]
            pieces = [mine[p * size : (p + 1) * size] for p in range(parts)]
            if step > 0:
                if number < len(every) - 1:
                    moved = swap(mine, "expert", step)
                    pieces = [moved[p * size : (p + 1) * size] for p in range(parts)]
                else:
                    pieces = [swap(p, "expert", step) for p in pieces]
            returned.append(pieces)

    mixed, summed = [], None
    for p in range(parts):
        if p > 0:
            returned[-1][p] = after(returned[-1][p], summed)
        summed = sum(r[p].astype(jnp.float32) for r in returned).astype(jnp.bfloat16)

        def piece(index):
            return lax.dynamic_slice_in_dim(summed, index * col_width, col_width, 1)

        result = piece(block).astype(jnp.float32)
        for step in range(1, blocks):
            moved = swap(piece(block ^ step), "ffn", 2 * step)
            result = result + moved.astype(jnp.float32)
        mixed.append(result.astype(jnp.bfloat16))
    return jnp.concatenate(mixed, axis=0)


def solution(mesh):
    in_specs = (
        P("expert", None),
        P("expert", None),
        P("expert", None),
        P("expert", None, "ffn"),
        P("expert", None, "ffn"),
        P("expert", "ffn", None),
    )
    out_specs = P("expert", "ffn")

    return jax.shard_map(
        per_device, mesh=mesh, in_specs=in_specs, out_specs=out_specs, check_vma=False
    )
```
